256 devices in a mesh: row: 4 (over x), col: 8 (over z), depth: 8 (over y, core).
Axes of the slice: x: 4, y: 4, z: 8, core: 2. Of those that a mesh axis runs over, the one named last changes fastest.
Arguments:
- trailing: float32 [1504, 48128], P('depth', ('row', 'col')), may hold values from -6 to 6
- panel_block: float32 [48128, 1024], P(('row', 'col', 'depth')), may hold values from -6 to 6
- factor_panel: float32 [48128, 1024], P(('row', 'col', 'depth')), may hold values from -0.1875 to 0.1875
- corner_block: float32 [1024, 1024], P(('row', 'col', 'depth')), may hold values from -6 to 6, as said below
- corner_inverse: float32 [1024, 1024], P(('row', 'col', 'depth')), may hold values from -1 to 2, as said below
Outputs:
- trailing_out: float32 [1504, 48128], P('depth', ('row', 'col'))
- panel_out: float32 [48128, 1024], P(('row', 'col', 'depth'))
- corner_out: float32 [1024, 1024], P(('row', 'col', 'depth'))
The draws below stay inside these ranges and needn't reach their ends.
Inputs may be any that keep to these rules, and one draw needn't show every extreme that they name: `corner_block`: symmetric. `corner_inverse`: lower triangular, diagonal between 1 and 2.
All inputs are finite; a program needn't handle non-finite values.
Results may differ from the reference program's by a relative error of at most 0.00012.
Values sent between devices are 32-bit elements; how exact they have to be, the bound alone decides.
No kernel may reach another device: no remote copies, remote signals or barrier semaphores. Data moves between devices by JAX's collectives and lax.ppermute only.
A program may use at most 128 MiB of HBM per device.

```python
import jax
import jax.numpy as jnp
from jax import lax

NB = 1024
M = 48128
SPAN = 1
SLAB = 1504
N_DEPTH = 8


def draw_corner_block(key, part):
    noise = jax.random.truncated_normal(jax.random.fold_in(key, 11), -4.0, 4.0, (NB, NB), jnp.float32)
    return (noise + noise.T) * 0.7071


def draw_corner_inverse(key, part):
    below = jax.random.truncated_normal(jax.random.fold_in(key, 23), -4.0, 4.0, (NB, NB), jnp.float32)
    diagonal = jax.random.uniform(jax.random.fold_in(key, 29), (NB,), jnp.float32, 1.0, 2.0)
    strict = jnp.tril(below, -1) * (0.5 / NB ** 0.5)
    return strict + jnp.diag(diagonal)


def block_scale(rng, shape, cuts, least, largest):
    level = 1.0
    for position, shards_of in cuts:
        draws = jax.random.uniform(jax.random.fold_in(jax.random.fold_in(rng, 6), position), (shards_of,), jnp.float32, least / len(cuts), largest / len(cuts))
        level = level * jnp.repeat(jnp.exp(draws), shape[position] // shards_of).reshape((-1,) + (1,) * (len(shape) - 1 - position))
    return level


def gaussian(stream_key, shape, scale, limit, cuts=(), dtype=jnp.bfloat16):
    loudness = block_scale(stream_key, shape, cuts, -0.22, 0.18) if cuts else 1.0
    array = jax.random.normal(stream_key, shape, jnp.float32) * scale * loudness
    return jnp.minimum(jnp.maximum(array, -limit), limit).astype(dtype)


def setup_inputs(seed: int = 0) -> dict:
    arg_keys = jax.random.split(jax.random.key(seed), 6)
    trailing = gaussian(arg_keys[0], (SLAB, M), 1.0, 6.0, ((0, 8), (1, 32)), jnp.float32)
    panel_block = gaussian(arg_keys[1], (M, NB), 1.0, 6.0, ((0, 256),), jnp.float32)
    factor_panel = gaussian(arg_keys[2], (M, NB), NB ** -0.5, 0.1875, ((0, 256),), jnp.float32)
    corner_block = draw_corner_block(jax.random.fold_in(arg_keys[5], 71), 0)
    corner_inverse = draw_corner_inverse(jax.random.fold_in(arg_keys[5], 71), 0)
    return dict(trailing=trailing, panel_block=panel_block, factor_panel=factor_panel, corner_block=corner_block, corner_inverse=corner_inverse)


def matmul(left, right):
    return jnp.dot(left, right, precision=lax.Precision.HIGHEST, preferred_element_type=jnp.float32)


def permute(matrix):
    block = matrix[:SLAB]
    shaped = block.reshape(SPAN, N_DEPTH, SLAB // (SPAN * N_DEPTH), block.shape[1])
    return jnp.transpose(shaped, (1, 0, 2, 3)).reshape(SLAB, block.shape[1])


def reference(trailing, panel_block, factor_panel, corner_block, corner_inverse):
    corner_out = matmul(corner_inverse, matmul(corner_block, corner_inverse.T))
    scaled = matmul(panel_block, corner_inverse.T)
    coupling = matmul(factor_panel, corner_out)
    half_panel = scaled - 0.5 * coupling
    panel_out = half_panel - 0.5 * coupling
    update = matmul(permute(half_panel), factor_panel.T) + matmul(permute(factor_panel), half_panel.T)
    trailing_out = trailing - update
    return trailing_out, panel_out, corner_out
```

```python
import jax
import jax.numpy as jnp
from jax import lax
from jax.sharding import PartitionSpec as P


NB = 1024
ROWS = 188
PAD = 192
HIGH = lax.Precision.HIGH


def dot(left, right):
    return lax.dot_general(left, right, (((1,), (0,)), ((), ())), precision=HIGH, preferred_element_type=jnp.float32)


def dot_t(left, right):
    return lax.dot_general(left, right, (((1,), (1,)), ((), ())), precision=HIGH, preferred_element_type=jnp.float32)


def y_shift(array, by):
    return lax.ppermute(array, "depth", [(d, (d + 2 * by) % 8) for d in range(8)])


def core_swap(array):
    return lax.ppermute(array, "depth", [(d, d ^ 1) for d in range(8)])


def z_shift(array, by):
    return lax.ppermute(array, "col", [(c, (c + by) % 8) for c in range(8)])


def x_shift(array, by):
    return lax.ppermute(array, "row", [(r, (r + by) % 4) for r in range(4)])


def place(parts, at):
    n = len(parts)
    out = jnp.zeros((n,) + parts[0].shape, parts[0].dtype)
    for k, part in enumerate(parts):
        out = lax.dynamic_update_index_in_dim(out, part, (at - k) % n, 0)
    return out


def pad_rows(array):
    return jnp.pad(array, ((0, PAD - array.shape[0]), (0, 0)))


def body(trailing, panel_block, factor_panel, corner_block, corner_inverse):
    r = lax.axis_index("row")
    c = lax.axis_index("col")
    d = lax.axis_index("depth")
    y, core = d // 2, d % 2
    first = core == 0

    row_id = 4 * ((r * 8 + c) * 8 + d) + lax.broadcasted_iota(jnp.int32, (4, NB), 0)
    col_id = lax.broadcasted_iota(jnp.int32, (4, NB), 1)
    packed = jnp.where(col_id <= row_id, corner_inverse, corner_block)
    diag = jnp.where(col_id == row_id, corner_block, 0.0).reshape(4, 8, 128).sum(1)
    low, high = packed[:, :512], packed[:, 512:]
    mine = jnp.concatenate([jnp.where(first, low, high), diag], 1)
    theirs = core_swap(jnp.concatenate([jnp.where(first, high, low), diag], 1))
    block = jnp.where(first, jnp.concatenate([mine, theirs]), jnp.concatenate([theirs, mine]))
    block = place([block, y_shift(block, 1), y_shift(block, 2), y_shift(block, -1)], y).reshape(32, 640)

    half = core_swap(jnp.where(first, factor_panel, panel_block))
    keep = jnp.where(first, panel_block, factor_panel)
    whole = jnp.where(first, jnp.concatenate([keep, half]), jnp.concatenate([half, keep]))
    top, bottom = whole[:PAD], whole[PAD:]
    left_top, right_bottom = y_shift(top, 1), y_shift(bottom, -1)
    left_bottom, right_top = y_shift(bottom, 1), y_shift(top, -1)

    slab = jnp.concatenate([pad_rows(factor_panel), pad_rows(panel_block)])
    pieces = [slab[48 * k : 48 * (k + 1)] for k in range(8)]
    piece = jnp.where(c == 0, pieces[0], 0.0)
    for k in range(1, 8):
        piece = piece + lax.ppermute(pieces[k], ("row", "col"), [(0, k)])

    block = place([block] + [z_shift(block, k) for k in range(1, 8)], c).reshape(256, 640)
    diag = block[:, 512:].reshape(2, 128, 128).sum(1)
    block = jnp.concatenate([block[:, :512], jnp.pad(diag, ((0, 6), (0, 384)))])

    left, right = x_shift(block, 1), x_shift(block, -1)
    across = jnp.concatenate([x_shift(left[:136], 1), x_shift(right[136:], -1)])

    piece_x = jnp.where(r == 0, piece, 0.0)
    for k in range(1, 4):
        piece_x = piece_x + lax.ppermute(piece, "row", [(0, k)])
    up, down, ring = piece_x, piece_x, [None] * 8
    ring[0] = piece_x
    for k in range(1, 5):
        up = z_shift(up, 1)
        ring[k] = up
        if k < 4:
            down = z_shift(down, -1)
            ring[8 - k] = down
    slab = place(ring, c).reshape(2 * PAD, NB)

    across_top, across_bottom = y_shift(left_top, 1), y_shift(right_bottom, -1)
    got = [
        whole,
        jnp.concatenate([left_top, left_bottom]),
        jnp.concatenate([across_top, across_bottom]),
        jnp.concatenate([right_top, right_bottom]),
    ]
    other = [core_swap(g) for g in got]
    got = place(got, y).reshape(8 * ROWS, NB)
    other = place(other, y).reshape(8 * ROWS, NB)

    halves = [block, left, across, right]
    swapped = [core_swap(h) for h in halves]
    halves, swapped = place(halves, r), place(swapped, r)
    low = jnp.where(first, halves, swapped)
    high = jnp.where(first, swapped, halves)
    diag = low[:, 256:258, :128].reshape(1, NB)
    packed = jnp.concatenate([low[:, :256].reshape(NB, 512), high[:, :256].reshape(NB, 512)], 1)
    rows = lax.broadcasted_iota(jnp.int32, (NB, NB), 0)
    cols = lax.broadcasted_iota(jnp.int32, (NB, NB), 1)
    inverse = jnp.where(cols <= rows, packed, 0.0)
    upper = jnp.where(cols > rows, packed, 0.0)
    corner = upper + upper.T + jnp.where(cols == rows, diag, 0.0)

    l_all = jnp.concatenate([pad_rows(factor_panel), slab[:PAD]])
    b_all = jnp.concatenate([pad_rows(panel_block), slab[PAD:]])
    u_all = dot(l_all, inverse)
    z_all = dot(jnp.concatenate([u_all, jnp.pad(corner_inverse, ((0, 4), (0, 0)))]), corner)
    t_all = jnp.concatenate([b_all - z_all[: 2 * PAD], z_all[2 * PAD :]])
    out = dot_t(t_all, inverse)
    panel_out = out[:ROWS]
    corner_out = out[2 * PAD : 2 * PAD + 4]
    panel_slab, u_slab = out[PAD : PAD + ROWS], u_all[PAD : PAD + ROWS]

    with_got = jnp.where(first, u_slab, panel_slab)
    with_other = jnp.where(first, panel_slab, u_slab)
    trailing_out = trailing - (dot_t(with_got, got) + dot_t(with_other, other))
    return trailing_out, panel_out, corner_out


def solution(mesh):
    rows = P(("row", "col", "depth"), None)
    in_specs = (P("depth", ("row", "col")), rows, rows, rows, rows)
    out_specs = (P("depth", ("row", "col")), rows, rows)
    return jax.shard_map(body, mesh=mesh, in_specs=in_specs, out_specs=out_specs, check_vma=False)
```
